16 devices in a mesh: rep: 2 (over y, z), dp: 8 (over x, core).
Axes of the slice: x: 4, y: 2, z: 1, core: 2. Of those that a mesh axis runs over, the one named last changes fastest.
The devices are a block of a 4x4x8 slice.
Arguments:
- x: bfloat16 [16, 2048, 768], P(('rep', 'dp')), parts along dimension 0
- dy: bfloat16 [16, 2048, 768], P(('rep', 'dp')), parts along dimension 0
- w_gate: bfloat16 [2, 768, 3072], P(None, 'dp')
- w_up: bfloat16 [2, 768, 3072], P(None, 'dp')
- w_down: bfloat16 [2, 3072, 768], P(None, 'dp')
Outputs:
- output 1: bfloat16 [16, 2048, 768], P(('rep', 'dp')), parts along dimension 0
- output 2: bfloat16 [4, 768, 3072], P('rep', 'dp'), parts along dimension 0
- output 3: bfloat16 [4, 768, 3072], P('rep', 'dp'), parts along dimension 0
- output 4: bfloat16 [4, 3072, 768], P('rep', 'dp'), parts along dimension 0
There are 2 independent parts. The reference program is written for one: setup_inputs(seed, part) draws one part's arguments, and reference() takes and returns one part's arrays. A program takes and returns all parts, laid end to end along the dimension named above; an argument that names none is the same for every part.
All inputs are finite; a program needn't handle non-finite values.
Results may differ from the reference program's by a relative error of at most 0.018.
Values are sent between devices in bfloat16 or wider.
A program may use at most 768 MiB of HBM per device.

```python
import jax
import jax.numpy as jnp
from jax import lax

SEQUENCES = 8
TOKENS = 2048
D = 768
FF = 3072
LAYERS = 2
NAMES = ("w_gate", "w_up", "w_down")
SHAPES = {"w_gate": (LAYERS, D, FF), "w_up": (LAYERS, D, FF), "w_down": (LAYERS, FF, D)}


def bump(key, n, height):
    away = (jnp.arange(n, dtype=jnp.int32) - jax.random.randint(key, (), 0, n, jnp.int32)) % n
    return jnp.where(away < n // 8, height, 1.0)


def together(key, own, strength):
    shared = jax.random.normal(key, own.shape[1:], jnp.float32)
    return (own + strength * shared) * lax.rsqrt(1 + strength * strength)


def setup_inputs(seed: int = 0, part: int = 0) -> dict:
    kx, kdy, ka, kb, kz, kf, kh, kl, *kw = jax.random.split(jax.random.key(seed), 8 + len(NAMES))
    kx, kdy, ka, kb = (jax.random.fold_in(k, part) for k in (kx, kdy, ka, kb))
    shape = (SEQUENCES, TOKENS, D)
    much_x, much_dy = jax.random.uniform(kz, (2,), jnp.float32, 0.0, 1.0)
    layers = 2.0 ** jax.random.uniform(kl, (LAYERS, 1, 1), jnp.float32, -1.0, 1.0)
    x = together(ka, jax.random.normal(kx, shape, jnp.float32), much_x) * bump(kf, D, 4.0)
    dy = together(kb, jax.random.normal(kdy, shape, jnp.float32), much_dy)
    drawn = {"x": x.astype(jnp.bfloat16), "dy": (dy * (SEQUENCES * TOKENS) ** -0.5).astype(jnp.bfloat16)}
    for key, name in zip(kw, NAMES, strict=True):
        w = jax.random.normal(key, SHAPES[name], jnp.float32) * SHAPES[name][1] ** -0.5
        drawn[name] = (w * {"w_gate": 1.0, "w_up": bump(kh, FF, 4.0), "w_down": layers}[name]).astype(jnp.bfloat16)
    return drawn


def matmul(a, w):
    return jnp.dot(a, w, preferred_element_type=jnp.float32).astype(jnp.bfloat16)


def normed(h):
    wide = h.astype(jnp.float32)
    scale = lax.rsqrt(jnp.mean(wide**2, -1, keepdims=True) + 1e-6)
    return (wide * scale).astype(jnp.bfloat16)


def layer(h, w):
    a = normed(h)
    gate = jnp.dot(a, w["w_gate"], preferred_element_type=jnp.float32)
    up = jnp.dot(a, w["w_up"], preferred_element_type=jnp.float32)
    return h + matmul((jax.nn.silu(gate) * up).astype(jnp.bfloat16), w["w_down"])


def stack(weights, h):
    return lax.scan(lambda h, w: (layer(h, w), None), h, weights)[0]


def reference(x, dy, w_gate, w_up, w_down):
    weights = dict(zip(NAMES, (w_gate, w_up, w_down), strict=True))

    def take(so_far, sequence):
        h, by_y = sequence
        _, back = jax.vjp(stack, weights, h)
        by_weights, by_h = back(by_y)
        return jax.tree.map(lambda total, term: total + term.astype(jnp.float32), so_far, by_weights), by_h

    none_yet = {name: jnp.zeros(w.shape, jnp.float32) for name, w in weights.items()}
    by_weights, by_x = lax.scan(take, none_yet, (x, dy))
    return (by_x, *(by_weights[name].astype(jnp.bfloat16) for name in NAMES))
```

```python
import functools

import jax
import jax.numpy as jnp
from jax import lax
from jax.experimental import pallas as pl
from jax.experimental.pallas import tpu as pltpu
from jax.sharding import PartitionSpec as P

MESH = pl.DeviceIdType.MESH
F32, BF16 = jnp.float32, jnp.bfloat16
LANES = 128
NT = (((1,), (1,)), ((), ()))
G, U, D = range(3)


def dot(a, b, dims=(((1,), (0,)), ((), ()))):
    return lax.dot_general(a, b, dims, preferred_element_type=F32)


def loop(n, body, unroll=1):
    def step(i, carry):
        body(i)
        return carry

    lax.fori_loop(0, n, step, 0, unroll=unroll)


def kernel(size, x_hbm, dy_hbm, wg_hbm, wu_hbm, wd_hbm,
           dx_hbm, og_hbm, ou_hbm, od_hbm, fg, fu, fd,
           own_g, own_u, own_d, sg, su, sd, h, a, at, dout, dt, da, act, dg, du,
           pg, pu, pd, sib_g, sib_u, sib_d, send_a_g, send_a_d, send_b_g, send_b_d,
           ra_g, ra_d, rb_g, rb_d, out_g, out_d,
           ag_send, ag_recv, own_sem, own_out, slot_sem, in_sem,
           sib_send, sib_recv, a_send, a_recv, b_send, b_recv, out_sem, credit):
    layers, chunks, rows, d, ff_chunk, tokens = (
        size[k] for k in ("layers", "chunks", "rows", "d", "ff_chunk", "tokens"))
    n = size["n"]
    chips = n // 2
    me = lax.axis_index("dp")
    x, c = me // 2, me % 2
    xr, xl, xo = lax.rem(x + 1, chips), lax.rem(x + chips - 1, chips), lax.rem(x + 2, chips)
    right, left, sibling = {"dp": xr * 2 + c}, {"dp": xl * 2 + c}, {"dp": x * 2 + 1 - c}
    units = layers * chunks

    barrier = pltpu.get_barrier_semaphore()
    for who in (left, right, sibling):
        pl.semaphore_signal(barrier, inc=1, device_id=who, device_id_type=MESH)

    R = (rows, rows, LANES)
    own, full, slot = (own_g, own_u, own_d), (fg, fu, fd), (sg, su, sd)

    def own_copies(q, m):
        l, k = q // chunks, q % chunks
        if m == D:
            return [pltpu.make_async_copy(wd_hbm.at[l, pl.ds(k * LANES, LANES)], own_d.at[q], own_sem.at[m, q, 0])]
        src = (wg_hbm, wu_hbm)[m]
        return [pltpu.make_async_copy(
            src.at[l, :, pl.ds((j * chunks + k) * LANES, LANES)], own[m].at[q, :, pl.ds(j * LANES, LANES)],
            own_sem.at[m, q, j]) for j in range(n)]

    def load_x(dst):
        return pltpu.make_async_copy(x_hbm.at[0], dst, in_sem.at[0])

    load_dy = pltpu.make_async_copy(dy_hbm.at[0], dout, in_sem.at[1])
    for q in range(units):
        for m in range(3):
            for cp in own_copies(q, m):
                cp.start()
        if q == 0:
            load_x(h).start()
            load_dy.start()

    def block(q, m, owner, half=None):
        start, size_ = owner * R[m], R[m]
        if half is not None:
            size_ = R[m] // 2
            start = start + half * size_
        return full[m].at[q, pl.ds(pl.multiple_of(start, 16), size_)]

    def remote(q, m, i, src, dst, to):
        return pltpu.make_async_remote_copy(src, dst, ag_send.at[q, m, i], ag_recv.at[q, m, i],
                                            device_id=to, device_id_type=MESH)

    def gather_copy(q, m, i):
        to = (right, left, sibling, right, sibling, left, sibling, sibling)[i]
        if i < 3:
            return remote(q, m, i, own[m].at[q], block(q, m, me), to)
        chip, half = ((xl, 0), (xl, None), (xr, 1), (xr, None), (xo, None))[i - 3]
        piece = block(q, m, chip * 2 + c, half)
        return remote(q, m, i, piece, piece, to)

    def own_store(q, m):
        return pltpu.make_async_copy(own[m].at[q], block(q, m, me), own_out.at[m, q])

    def g0(q, m):
        for i in range(3):
            gather_copy(q, m, i).start()
        own_store(q, m).start()

    def g1(q, m):
        for came in range(2):
            gather_copy(q, m, came).wait_recv()
            gather_copy(q, m, 3 + 2 * came).start()
            gather_copy(q, m, 4 + 2 * came).start()

    def g2(q, m):
        gather_copy(q, m, 3).wait_recv()
        gather_copy(q, m, 5).wait_recv()
        gather_copy(q, m, 7).start()

    def g3(q, m):
        for i in (2, 4, 6, 7):
            gather_copy(q, m, i).wait_recv()
        own_store(q, m).wait()

    def g_end(q, m):
        for i in range(8):
            gather_copy(q, m, i).wait_send()

    def fetch(q, s, m):
        return pltpu.make_async_copy(full[m].at[q], slot[m].at[s], slot_sem.at[s, m])

    TP = 256
    prep_tiles = tokens // TP

    def scale_of(wide):
        return lax.rsqrt(jnp.mean(wide * wide, -1, keepdims=True) + 1e-6)

    def norm_tile(i):
        r = pl.ds(i * TP, TP)
        wide = h[r, :].astype(F32)
        a_tile = (wide * scale_of(wide)).astype(BF16)
        a[r, :] = a_tile
        return a_tile

    def transpose_a(i):
        cols = pl.ds(pl.multiple_of(i * TP, TP), TP)
        at[:, cols] = norm_tile(i).T

    def transpose_dout(i):
        cols = pl.ds(pl.multiple_of(i * TP, TP), TP)
        dt[:, cols] = dout[pl.ds(i * TP, TP), :].T

    T, NB = 512, 256
    tiles, blocks = tokens // T, ff_chunk // NB

    def forward_tile(s, i, first):
        r = pl.ds(i * T, T)
        a_tile = a[r, :]
        gate = dot(a_tile, sg[s])
        up = dot(a_tile, su[s])
        hidden = (gate * jax.nn.sigmoid(gate) * up).astype(BF16)
        term = dot(hidden, sd[s])

        @pl.when(first)
        def _():
            da[r, :] = term

        @pl.when(jnp.logical_not(first))
        def _():
            da[r, :] += term

    def hidden_tile(s, i):
        r = pl.ds(pl.multiple_of((i % tiles) * T, T), T)
        f = pl.ds(pl.multiple_of((i // tiles) * NB, NB), NB)
        a_tile = a[r, :]
        gate = dot(a_tile, sg[s, :, f])
        up = dot(a_tile, su[s, :, f])
        by_hidden = dot(dout[r, :], sd[s, f, :], NT).astype(BF16).astype(F32)
        sig = jax.nn.sigmoid(gate)
        silu = gate * sig
        act[r, f] = (silu * up).astype(BF16)
        du[r, f] = (by_hidden * silu).astype(BF16)
        dg[r, f] = (by_hidden * up * (sig + silu * (1.0 - sig))).astype(BF16)

    def weights_up(b, src, dst):
        f = pl.ds(pl.multiple_of(b * NB, NB), NB)
        term = dot(at[...], src[:, f]).astype(BF16)
        dst[:, :, f] = term.reshape(chips, 2 * rows, NB)

    def weights_down(b):
        f = pl.ds(pl.multiple_of(b * NB, NB), NB)
        term = dot(dt[...], act[:, f])
        pd[b] = term.T.astype(BF16)

    def input_tile(s, i, first):
        r = pl.ds(i * T, T)
        term = dot(dg[r, :], sg[s], NT) + dot(du[r, :], su[s], NT)

        @pl.when(first)
        def _():
            da[r, :] = term

        @pl.when(jnp.logical_not(first))
        def _():
            da[r, :] += term

    def norm_back(i):
        r = pl.ds(i * TP, TP)
        wide = h[r, :].astype(F32)
        s = scale_of(wide)
        g = da[r, :].astype(BF16).astype(F32)
        along = jnp.sum(g * wide, -1, keepdims=True)
        back = (g * s - wide * (s * s * s * along * (1.0 / d))).astype(BF16)
        dout[r, :] = (dout[r, :].astype(F32) + back.astype(F32)).astype(BF16)

    part, sib = (pg, pu, pd), (sib_g, sib_u, sib_d)
    view = lambda pair, m: pair[0].at[m] if m != D else pair[1]
    sa = [view((send_a_g, send_a_d), m) for m in range(3)]
    ra = [[r_.at[i] for i in range(2)] for r_ in (view((ra_g, ra_d), m) for m in range(3))]
    sb = [[r_.at[i] for i in range(2)] for r_ in (view((send_b_g, send_b_d), m) for m in range(3))]
    rb = [[r_.at[i] for i in range(2)] for r_ in (view((rb_g, rb_d), m) for m in range(3))]
    out = [view((out_g, out_d), m) for m in range(3)]

    def rs_sib(m):
        return pltpu.make_async_remote_copy(
            part[m].at[:, pl.ds(pl.multiple_of((1 - c) * R[m], 16), R[m])], sib[m], sib_send.at[m], sib_recv.at[m],
            device_id=sibling, device_id_type=MESH)

    def rs_a(m, i):
        half = R[m] // 2
        return pltpu.make_async_remote_copy(
            sa[m].at[pl.ds(i * half, half)], ra[m][i], a_send.at[m, i], a_recv.at[m, i],
            device_id=(right, left)[i], device_id_type=MESH)

    def rs_b(m, i):
        return pltpu.make_async_remote_copy(
            sb[m][i], rb[m][i], b_send.at[m, i], b_recv.at[m, i],
            device_id=(right, left)[i], device_id_type=MESH)

    def term(m, chip):
        mine = part[m][chip, pl.ds(pl.multiple_of(c * R[m], 16), R[m]), :]
        return mine.astype(F32) + sib[m][chip].astype(F32)

    def rs1(s, m):
        @pl.when(s > 0)
        def _():
            pl.semaphore_wait(credit.at[m], 1)

        rs_sib(m).start()

    def rs2(s, m):
        rs_sib(m).wait()
        sa[m][...] = term(m, xo).astype(BF16)
        for i in range(2):
            rs_a(m, i).start()

    def rs3(m):
        half = R[m] // 2
        for i in range(2):
            rs_a(m, i).wait()
        for i, chip in enumerate((xr, xl)):
            whole = term(m, chip)
            came = ra[m][i][...].astype(F32)
            top, low = whole[:half], whole[half:]
            if i == 0:
                top = top + came
            else:
                low = low + came
            sb[m][i][:half, :] = top.astype(BF16)
            sb[m][i][half:, :] = low.astype(BF16)
        for i in range(2):
            rs_b(m, i).start()

    def out_copies(s, m):
        l, k = layers - 1 - s // chunks, lax.rem(s, chunks)
        if m == D:
            return [pltpu.make_async_copy(out[m], od_hbm.at[l, pl.ds(k * LANES, LANES)], out_sem.at[m, 0])]
        dst = (og_hbm, ou_hbm)[m]
        return [pltpu.make_async_copy(
            out[m].at[:, pl.ds(j * LANES, LANES)],
            dst.at[l, :, pl.ds(pl.multiple_of((j * chunks + k) * LANES, LANES), LANES)], out_sem.at[m, j])
            for j in range(n)]

    def rs4(s, m):
        @pl.when(s > 0)
        def _():
            for cp in out_copies(s, m):
                cp.wait()

        for i in range(2):
            rs_b(m, i).wait()
        total = term(m, x) + rb[m][0][...].astype(F32) + rb[m][1][...].astype(F32)
        out[m][...] = total.astype(BF16)
        for cp in out_copies(s, m):
            cp.start()

        @pl.when(s < units - 1)
        def _():
            pl.semaphore_signal(credit.at[m], inc=1, device_id=sibling, device_id_type=MESH)

    for m in range(3):
        for cp in own_copies(0, m):
            cp.wait()
    pl.semaphore_wait(barrier, 3)
    for m in range(3):
        g0(0, m)
    for q in range(1, units):
        for m in range(3):
            for cp in own_copies(q, m):
                cp.wait()
    load_x(h).wait()
    loop(prep_tiles, norm_tile)
    load_dy.wait()
    loop(prep_tiles, transpose_dout)

    def finish_gather(q, s):
        for m in range(3):
            g2(q, m)
        for m in range(3):
            g3(q, m)
            fetch(q, s, m).start()

    for m in range(3):
        g1(0, m)
    for m in range(3):
        g0(1, m)
    finish_gather(0, 0)

    def forward(k, carry):
        s = lax.rem(k, 2)
        for m in range(3):
            fetch(k, s, m).wait()

        def tile(i):
            for m in range(2):
                @pl.when(i == 1 + 2 * m)
                def _():
                    g1(k + 1, m)

            forward_tile(s, i, k == 0)

        loop(tiles, tile)
        g1(k + 1, D)
        for m in range(3):
            g0(k + 2, m)
        finish_gather(k + 1, lax.rem(k + 1, 2))
        return carry

    fwd = units - chunks
    lax.fori_loop(0, fwd, forward, 0)

    def add_hidden(i):
        r = pl.ds(i * TP, TP)
        h[r, :] = (h[r, :].astype(F32) + da[r, :].astype(BF16).astype(F32)).astype(BF16)

    loop(prep_tiles, add_hidden)
    loop(prep_tiles, transpose_a)

    def backward(k, carry):
        s = lax.rem(k + fwd, 2)
        q_next = lax.rem(k + fwd + 1, units)
        more = k < units - fwd - 1
        first = lax.rem(k, chunks) == 0

        @pl.when(jnp.logical_and(first, k > 0))
        def _():
            load_x(h).wait()
            loop(prep_tiles, transpose_a)
            loop(prep_tiles, transpose_dout)

        @pl.when(k > 0)
        def _():
            for m in range(3):
                rs3(m)

        for m in range(3):
            fetch(0, s, m).wait()

        def tile(i):
            for m in range(3):
                @pl.when(jnp.logical_and(more, i == 1 + 6 * m))
                def _():
                    g1(q_next, m)

            hidden_tile(s, i)

        loop(tiles * blocks, tile)

        @pl.when(k < units - fwd - 2)
        def _():
            for m in range(3):
                g0(q_next + 1, m)

        @pl.when(k > 0)
        def _():
            for m in range(3):
                rs4(k - 1, m)

        loop(blocks, lambda b: weights_up(b, dg, pg))
        rs1(k, G)
        loop(blocks, lambda b: weights_up(b, du, pu))
        rs1(k, U)
        rs2(k, G)

        @pl.when(more)
        def _():
            for m in range(3):
                g2(q_next, m)

        loop(blocks, weights_down)
        rs1(k, D)
        rs2(k, U)

        @pl.when(more)
        def _():
            for m in range(3):
                g3(q_next, m)

        @pl.when(k < units - 1)
        def _():
            for m in range(3):
                fetch(q_next, 1 - s, m).start()

        def back(i):
            @pl.when(i == 1)
            def _():
                rs2(k, D)

            input_tile(s, i, first)

        loop(tiles, back)

        @pl.when(lax.rem(k, chunks) == chunks - 1)
        def _():
            loop(prep_tiles, norm_back)

            @pl.when(k < units - 1)
            def _():
                load_x(h).start()

        return carry

    lax.fori_loop(0, units, backward, 0)
    store_dx = pltpu.make_async_copy(dout, dx_hbm.at[0], in_sem.at[1])
    store_dx.start()
    for m in range(3):
        rs3(m)
    for m in range(3):
        rs4(units - 1, m)
    for m in range(3):
        for cp in out_copies(units - 1, m):
            cp.wait()
    store_dx.wait()

    def ends(q):
        for m in range(3):
            g_end(q, m)

    loop(units, ends)


def solution(mesh):
    n = mesh.shape["dp"]

    def step(x, dy, wg, wu, wd):
        layers, rows, ff = wg.shape
        tokens, d = x.shape[1:]
        chunks = ff // (n * LANES)
        ff_chunk = n * LANES
        units = layers * chunks
        chips = n // 2
        size = dict(layers=layers, chunks=chunks, rows=rows, d=d, ff_chunk=ff_chunk, tokens=tokens, n=n)
        sds = jax.ShapeDtypeStruct
        vm = pltpu.VMEM
        dma = pltpu.SemaphoreType.DMA
        hbm = pl.BlockSpec(memory_space=pl.ANY)
        td = (tokens, d)
        tf = (tokens, ff_chunk)
        up, down = (rows, ff_chunk), (LANES, d)
        scratch = [
            vm((units, *up), BF16), vm((units, *up), BF16), vm((units, *down), BF16),
            vm((2, d, ff_chunk), BF16), vm((2, d, ff_chunk), BF16), vm((2, ff_chunk, d), BF16),
            vm(td, BF16), vm(td, BF16), vm(td[::-1], BF16), vm(td, BF16), vm(td[::-1], BF16), vm(td, F32),
            vm(tf, BF16), vm(tf, BF16), vm(tf, BF16),
            vm((chips, 2 * rows, ff_chunk), BF16), vm((chips, 2 * rows, ff_chunk), BF16), vm((chips, 2 * LANES, d), BF16),
            vm((chips, *up), BF16), vm((chips, *up), BF16), vm((chips, *down), BF16),
            vm((2, *up), BF16), vm(down, BF16), vm((2, 2, *up), BF16), vm((2, *down), BF16),
            vm((2, 2, rows // 2, ff_chunk), BF16), vm((2, LANES // 2, d), BF16), vm((2, 2, *up), BF16), vm((2, *down), BF16),
            vm((2, *up), BF16), vm(down, BF16),
            dma((units, 3, 8)), dma((units, 3, 8)), dma((3, units, n)), dma((3, units)), dma((2, 3)), dma((2,)),
            dma((3,)), dma((3,)), dma((3, 2)), dma((3, 2)), dma((3, 2)), dma((3, 2)), dma((3, n)),
            pltpu.SemaphoreType.REGULAR((3,)),
        ]
        outs = pl.pallas_call(
            functools.partial(kernel, size),
            out_shape=[
                sds(x.shape, BF16), sds(wg.shape, BF16), sds(wu.shape, BF16), sds(wd.shape, BF16),
                sds((units, d, ff_chunk), BF16), sds((units, d, ff_chunk), BF16), sds((units, ff_chunk, d), BF16),
            ],
            in_specs=[hbm] * 5,
            out_specs=[hbm] * 7,
            scratch_shapes=scratch,
            compiler_params=pltpu.CompilerParams(
                collective_id=0, has_side_effects=True, vmem_limit_bytes=67_043_328),
            name="stack",
        )(x, dy, wg, wu, wd)
        return tuple(outs[:4])

    seq, w = P(("rep", "dp"), None, None), P(None, "dp", None)
    return jax.shard_map(step, mesh=mesh, in_specs=(seq, seq, w, w, w),
                         out_specs=(seq, *(P("rep", "dp", None),) * 3), check_vma=False)
```

```python
import functools

import jax
import jax.numpy as jnp
from jax import lax
from jax.experimental import pallas as pl
from jax.experimental.pallas import tpu as pltpu
from jax.sharding import PartitionSpec as P

MESH = pl.DeviceIdType.MESH
F32, BF16 = jnp.float32, jnp.bfloat16
LANES = 128
NT = (((1,), (1,)), ((), ()))
G, U, D = range(3)


def dot(a, b, dims=(((1,), (0,)), ((), ()))):
    return lax.dot_general(a, b, dims, preferred_element_type=F32)


def loop(n, body, unroll=1):
    def step(i, carry):
        body(i)
        return carry

    lax.fori_loop(0, n, step, 0, unroll=unroll)


def kernel(size, x_hbm, dy_hbm, wg_hbm, wu_hbm, wd_hbm,
           dx_hbm, og_hbm, ou_hbm, od_hbm, fg, fu, fd,
           own_g, own_u, own_d, sgu, sd, h, a, at, dout, dt, da, act, dgu,
           pg, pu, pd, sib_g, sib_u, sib_d, send_a_g, send_a_d, send_b_g, send_b_d,
           ra_g, ra_d, rb_g, rb_d, out_g, out_d,
           ag_send, ag_recv, own_sem, own_out, slot_sem, in_sem,
           sib_send, sib_recv, a_send, a_recv, b_send, b_recv, out_sem, credit):
    layers, chunks, rows, d, ff_chunk, tokens = (
        size[k] for k in ("layers", "chunks", "rows", "d", "ff_chunk", "tokens"))
    n = size["n"]
    chips = n // 2
    me = lax.axis_index("dp")
    x, c = me // 2, me % 2
    xr, xl, xo = lax.rem(x + 1, chips), lax.rem(x + chips - 1, chips), lax.rem(x + 2, chips)
    right, left, sibling = {"dp": xr * 2 + c}, {"dp": xl * 2 + c}, {"dp": x * 2 + 1 - c}
    units = layers * chunks

    barrier = pltpu.get_barrier_semaphore()
    other = {"rep": lax.axis_index("rep") + 1 - 2 * (lax.axis_index("rep") % 2)}
    for who in (left, right, sibling, other):
        pl.semaphore_signal(barrier, inc=1, device_id=who, device_id_type=MESH)

    R = (rows, rows, LANES)
    own, full = (own_g, own_u, own_d), (fg, fu, fd)
    sg, su = (sgu.at[:, :, pl.ds(i * ff_chunk, ff_chunk)] for i in range(2))
    dg, du = (dgu.at[:, pl.ds(i * ff_chunk, ff_chunk)] for i in range(2))
    slot = (sg, su, sd)

    def own_copies(q, m):
        l, k = q // chunks, q % chunks
        if m == D:
            return [pltpu.make_async_copy(wd_hbm.at[l, pl.ds(k * LANES, LANES)], own_d.at[q], own_sem.at[m, q, 0])]
        src = (wg_hbm, wu_hbm)[m]
        return [pltpu.make_async_copy(
            src.at[l, :, pl.ds((j * chunks + k) * LANES, LANES)], own[m].at[q, :, pl.ds(j * LANES, LANES)],
            own_sem.at[m, q, j]) for j in range(n)]

    def load_x(dst):
        return pltpu.make_async_copy(x_hbm.at[0], dst, in_sem.at[0])

    load_dy = pltpu.make_async_copy(dy_hbm.at[0], dout, in_sem.at[1])

    S = tuple(r // 3 // 16 * 16 for r in R)
    pair = lax.axis_index("rep") % 2
    partner = {"rep": lax.axis_index("rep") + 1 - 2 * pair}

    def block(q, m, owner, start, count):
        return full[m].at[q, pl.ds(pl.multiple_of(owner * R[m] + start, 16), count)]

    def gather_copy(q, m, i):
        to = (right, left, sibling, right, sibling, left, sibling, sibling,
              partner, partner, partner, sibling, sibling, sibling)[i]
        ours, both = pair * S[m], R[m] - S[m]
        if i < 2:
            src, dst = own[m].at[q, pl.ds(pl.multiple_of(ours, 16), both)], block(q, m, me, ours, both)
        elif i == 2:
            src, dst = own[m].at[q], block(q, m, me, 0, R[m])
        else:
            owner = (xl, xl, xr, xr, xo, xl, xr, xo, xl, xr, xo)[i - 3] * 2 + c
            if i == 3:
                piece = (ours, both // 2)
            elif i == 5:
                piece = (ours + both // 2, both // 2)
            elif i < 8:
                piece = (ours, both)
            elif i < 11:
                piece = (pair * both, S[m])
            else:
                piece = ((1 - pair) * both, S[m])
            src = dst = block(q, m, owner, *piece)
        return pltpu.make_async_remote_copy(src, dst, ag_send.at[q, m, i], ag_recv.at[q, m, i],
                                            device_id=to, device_id_type=MESH)

    def own_store(q, m):
        return pltpu.make_async_copy(own[m].at[q], block(q, m, me, 0, R[m]), own_out.at[m, q])

    def g0(q):
        for m in range(3):
            for i in range(3):
                gather_copy(q, m, i).start()
            own_store(q, m).start()

    def g1(q, m):
        for came in range(2):
            gather_copy(q, m, came).wait_recv()
            for i in (3 + 2 * came, 8 + came, 4 + 2 * came):
                gather_copy(q, m, i).start()

    def g2(q, m):
        gather_copy(q, m, 3).wait_recv()
        gather_copy(q, m, 5).wait_recv()
        gather_copy(q, m, 10).start()
        gather_copy(q, m, 7).start()

    def g3(q, m):
        for i in range(3):
            gather_copy_from_partner(q, m, i).wait_recv()
            gather_copy(q, m, 11 + i).start()

    def gather_copy_from_partner(q, m, i):
        owner = (xl, xr, xo)[i] * 2 + c
        piece = block(q, m, owner, (1 - pair) * (R[m] - S[m]), S[m])
        return pltpu.make_async_remote_copy(piece, piece, ag_send.at[q, m, 8 + i], ag_recv.at[q, m, 8 + i],
                                            device_id=partner, device_id_type=MESH)

    def g4(q):
        for m in range(3):
            for i in (2, 4, 6, 7, 11, 12, 13):
                gather_copy(q, m, i).wait_recv()
            own_store(q, m).wait()

    def g_end(q, m):
        for i in range(14):
            gather_copy(q, m, i).wait_send()

    last = units - 1

    def gather_part(q, i):
        if i == 1:
            @pl.when(q < last)
            def _():
                g1(q, D)
                g0(q + 1)
        elif 2 <= i < 5:
            g2(q, i - 2)
        elif i >= 5:
            g3(q, i - 5)

            if i == 6:
                @pl.when(q < last)
                def _():
                    g1(q + 1, G)

    def gather_end(q, s):
        g4(q)
        for m in range(3):
            fetch(q, s, m).start()

        @pl.when(q < last - 1)
        def _():
            g1(q + 1, U)

    def fetch(q, s, m):
        return pltpu.make_async_copy(full[m].at[q], slot[m].at[s], slot_sem.at[s, m])

    TP = 256
    prep_tiles = tokens // TP

    def scale_of(wide):
        return lax.rsqrt(jnp.mean(wide * wide, -1, keepdims=True) + 1e-6)

    def norm_tile(i, src=h):
        r = pl.ds(i * TP, TP)
        wide = src[r, :].astype(F32)
        a_tile = (wide * scale_of(wide)).astype(BF16)
        a[r, :] = a_tile
        return a_tile

    def transpose_a(i):
        cols = pl.ds(pl.multiple_of(i * TP, TP), TP)
        at[:, cols] = norm_tile(i).T

    def restart(i):
        r = pl.ds(i * TP, TP)
        cols = pl.ds(pl.multiple_of(i * TP, TP), TP)
        h[r, :] = a[r, :]
        at[:, cols] = norm_tile(i, a).T
        dt[:, cols] = dout[r, :].T

    def transpose_dout(i):
        cols = pl.ds(pl.multiple_of(i * TP, TP), TP)
        dt[:, cols] = dout[pl.ds(i * TP, TP), :].T

    T, NB = 512, 1024
    TI = 512
    TH, NH = 1024, 256
    strips = ff_chunk // NH
    spots = strips * (tokens // TH)
    tiles, blocks = tokens // T, ff_chunk // NB

    def forward_tile(s, i, first):
        r = pl.ds(i * T, T)
        a_tile = a[r, :]
        gate = dot(a_tile, sg[s])
        up = dot(a_tile, su[s])
        hidden = (gate * jax.nn.sigmoid(gate) * up).astype(BF16)
        term = dot(hidden, sd[s])

        da[r, :] = jnp.where(first, 0.0, da[r, :]) + term

    def hidden_tile(s, i, b):
        r = pl.ds(pl.multiple_of(i * TH, TH), TH)
        f = pl.ds(pl.multiple_of(b * NH, NH), NH)
        a_tile = a[r, :]
        gate = dot(a_tile, sg[s, :, f])
        up = dot(a_tile, su[s, :, f])
        by_hidden = dot(dout[r, :], sd[s, f, :], NT).astype(BF16).astype(F32)
        sig = jax.nn.sigmoid(gate)
        silu = gate * sig
        act[r, f] = (silu * up).astype(BF16)
        du[r, f] = (by_hidden * silu).astype(BF16)
        dg[r, f] = (by_hidden * up * (sig + silu * (1.0 - sig))).astype(BF16)

    def weights_up(b, src, dst):
        f = pl.ds(pl.multiple_of(b * NB, NB), NB)
        term = dot(at[...], src[:, f]).astype(BF16)
        dst[:, :, f] = term.reshape(chips, 2 * rows, NB)

    def weights_down(b):
        f = pl.ds(pl.multiple_of(b * NB, NB), NB)
        term = dot(dt[...], act[:, f])
        per = NB // (2 * LANES)
        pd[pl.ds(b * per, per)] = term.T.astype(BF16).reshape(per, 2 * LANES, d)

    def input_tile(s, i, first):
        r = pl.ds(i * TI, TI)
        term = dot(dgu[r, :], sgu[s], NT)

        da[r, :] = jnp.where(first, 0.0, da[r, :]) + term

    def norm_back(i):
        r = pl.ds(i * TP, TP)
        wide = h[r, :].astype(F32)
        s = scale_of(wide)
        g = da[r, :].astype(BF16).astype(F32)
        along = jnp.sum(g * wide, -1, keepdims=True)
        back = (g * s - wide * (s * s * s * along * (1.0 / d))).astype(BF16)
        dout[r, :] = (dout[r, :].astype(F32) + back.astype(F32)).astype(BF16)

    part, sib = (pg, pu, pd), (sib_g, sib_u, sib_d)
    view = lambda pair, m: pair[0].at[m] if m != D else pair[1]
    sa = [view((send_a_g, send_a_d), m) for m in range(3)]
    ra = [[r_.at[i] for i in range(2)] for r_ in (view((ra_g, ra_d), m) for m in range(3))]
    sb = [[r_.at[i] for i in range(2)] for r_ in (view((send_b_g, send_b_d), m) for m in range(3))]
    rb = [[r_.at[i] for i in range(2)] for r_ in (view((rb_g, rb_d), m) for m in range(3))]
    out = [view((out_g, out_d), m) for m in range(3)]

    def rs_sib(m):
        return pltpu.make_async_remote_copy(
            part[m].at[:, pl.ds(pl.multiple_of((1 - c) * R[m], 16), R[m])], sib[m], sib_send.at[m], sib_recv.at[m],
            device_id=sibling, device_id_type=MESH)

    def rs_a(m, i):
        half = R[m] // 2
        return pltpu.make_async_remote_copy(
            sa[m].at[pl.ds(i * half, half)], ra[m][i], a_send.at[m, i], a_recv.at[m, i],
            device_id=(right, left)[i], device_id_type=MESH)

    def rs_b(m, i):
        return pltpu.make_async_remote_copy(
            sb[m][i], rb[m][i], b_send.at[m, i], b_recv.at[m, i],
            device_id=(right, left)[i], device_id_type=MESH)

    def term(m, chip):
        mine = part[m][chip, pl.ds(pl.multiple_of(c * R[m], 16), R[m]), :]
        return mine.astype(F32) + sib[m][chip].astype(F32)

    def rs1(s, m):
        @pl.when(s > 0)
        def _():
            pl.semaphore_wait(credit.at[m], 1)

        rs_sib(m).start()

    def rs2(s, m):
        rs_sib(m).wait()
        sa[m][...] = term(m, xo).astype(BF16)
        for i in range(2):
            rs_a(m, i).start()

    def rs3(m):
        half = R[m] // 2
        for i in range(2):
            rs_a(m, i).wait()
        for i, chip in enumerate((xr, xl)):
            whole = term(m, chip)
            came = ra[m][i][...].astype(F32)
            top, low = whole[:half], whole[half:]
            if i == 0:
                top = top + came
            else:
                low = low + came
            sb[m][i][:half, :] = top.astype(BF16)
            sb[m][i][half:, :] = low.astype(BF16)
        for i in range(2):
            rs_b(m, i).start()

    def out_copies(s, m):
        l, k = layers - 1 - s // chunks, lax.rem(s, chunks)
        if m == D:
            return [pltpu.make_async_copy(out[m], od_hbm.at[l, pl.ds(k * LANES, LANES)], out_sem.at[m, 0])]
        dst = (og_hbm, ou_hbm)[m]
        return [pltpu.make_async_copy(
            out[m].at[:, pl.ds(j * LANES, LANES)],
            dst.at[l, :, pl.ds(pl.multiple_of((j * chunks + k) * LANES, LANES), LANES)], out_sem.at[m, j])
            for j in range(n)]

    def rs4(s, m):
        @pl.when(s > 0)
        def _():
            for cp in out_copies(s, m):
                cp.wait()

        for i in range(2):
            rs_b(m, i).wait()
        total = term(m, x) + rb[m][0][...].astype(F32) + rb[m][1][...].astype(F32)
        out[m][...] = total.astype(BF16)
        for cp in out_copies(s, m):
            cp.start()

        @pl.when(s < units - 1)
        def _():
            pl.semaphore_signal(credit.at[m], inc=1, device_id=sibling, device_id_type=MESH)

    for m in range(3):
        for cp in own_copies(0, m):
            cp.start()
    load_x(h).start()
    load_dy.start()
    for m in range(3):
        for cp in own_copies(0, m):
            cp.wait()
    pl.semaphore_wait(barrier, 4)
    g0(0)
    for q in range(1, units):
        for m in range(3):
            for cp in own_copies(q, m):
                cp.start()
    for q in range(1, units):
        for m in range(3):
            for cp in own_copies(q, m):
                cp.wait()
    load_x(h).wait()
    loop(prep_tiles, norm_tile)
    load_dy.wait()
    loop(prep_tiles, transpose_dout)
    g1(0, G)
    g1(0, U)
    for i in range(8):
        gather_part(0, i)
    gather_end(0, 0)

    def forward(k, carry):
        s = lax.rem(k, 2)
        for m in range(3):
            fetch(k, s, m).wait()

        def tile(i):
            for j in range(8):
                @pl.when(i == j * tiles // 8)
                def _():
                    gather_part(k + 1, j)

            forward_tile(s, i, k == 0)

        loop(tiles, tile)
        gather_end(k + 1, 1 - s)
        return carry

    fwd = units - chunks
    lax.fori_loop(0, fwd, forward, 0)

    def add_hidden(i):
        r = pl.ds(i * TP, TP)
        h[r, :] = (h[r, :].astype(F32) + da[r, :].astype(BF16).astype(F32)).astype(BF16)

    loop(prep_tiles, add_hidden)
    loop(prep_tiles, transpose_a)

    def backward(k, carry):
        s = lax.rem(k + fwd, 2)
        q_next = lax.rem(k + fwd + 1, units)
        more = k < units - fwd - 1
        first = lax.rem(k, chunks) == 0

        @pl.when(jnp.logical_and(first, k > 0))
        def _():
            load_x(a).wait()
            loop(prep_tiles, restart)

        for m in range(3):
            fetch(0, s, m).wait()

        def strip(b):
            for j in range(8):
                @pl.when(jnp.logical_and(more, b == j * strips // 8))
                def _():
                    gather_part(q_next, j)

            for i in range(tokens // TH):
                hidden_tile(s, i, b)

        loop(strips, strip)

        @pl.when(k > 0)
        def _():
            for m in range(3):
                rs4(k - 1, m)

        @pl.when(jnp.logical_and(lax.rem(k, chunks) == chunks - 1, k < units - 1))
        def _():
            load_x(a).start()

        loop(blocks, lambda b: weights_up(b, dg, pg))
        rs1(k, G)

        @pl.when(jnp.logical_and(more, q_next == last - 1))
        def _():
            g1(last, U)
            g1(last, D)

        loop(blocks, lambda b: weights_up(b, du, pu))
        rs1(k, U)
        rs2(k, G)

        loop(blocks, weights_down)
        rs1(k, D)
        rs2(k, U)

        @pl.when(more)
        def _():
            gather_end(q_next, 1 - s)

        @pl.when(jnp.logical_and(k < units - 1, jnp.logical_not(more)))
        def _():
            for m in range(3):
                fetch(q_next, 1 - s, m).start()

        def back(i):
            @pl.when(i == 1)
            def _():
                rs2(k, D)
                rs3(G)

            @pl.when(i == 2)
            def _():
                rs3(U)

            input_tile(s, i, first)

        loop(tokens // TI, back)
        rs3(D)

        @pl.when(lax.rem(k, chunks) == chunks - 1)
        def _():
            loop(prep_tiles, norm_back)


        return carry

    lax.fori_loop(0, units, backward, 0)
    store_dx = pltpu.make_async_copy(dout, dx_hbm.at[0], in_sem.at[1])
    store_dx.start()
    for m in range(3):
        rs4(units - 1, m)
    for m in range(3):
        for cp in out_copies(units - 1, m):
            cp.wait()
    store_dx.wait()

    def ends(q):
        for m in range(3):
            g_end(q, m)

    loop(units, ends)


def solution(mesh):
    n = mesh.shape["dp"]

    def step(x, dy, wg, wu, wd):
        layers, rows, ff = wg.shape
        tokens, d = x.shape[1:]
        chunks = ff // (n * LANES)
        ff_chunk = n * LANES
        units = layers * chunks
        chips = n // 2
        size = dict(layers=layers, chunks=chunks, rows=rows, d=d, ff_chunk=ff_chunk, tokens=tokens, n=n)
        sds = jax.ShapeDtypeStruct
        vm = pltpu.VMEM
        dma = pltpu.SemaphoreType.DMA
        hbm = pl.BlockSpec(memory_space=pl.ANY)
        td = (tokens, d)
        tf = (tokens, ff_chunk)
        up, down = (rows, ff_chunk), (LANES, d)
        scratch = [
            vm((units, *up), BF16), vm((units, *up), BF16), vm((units, *down), BF16),
            vm((2, d, 2 * ff_chunk), BF16), vm((2, ff_chunk, d), BF16),
            vm(td, BF16), vm(td, BF16), vm(td[::-1], BF16), vm(td, BF16), vm(td[::-1], BF16), vm(td, F32),
            vm(tf, BF16), vm((tokens, 2 * ff_chunk), BF16),
            vm((chips, 2 * rows, ff_chunk), BF16), vm((chips, 2 * rows, ff_chunk), BF16), vm((chips, 2 * LANES, d), BF16),
            vm((chips, *up), BF16), vm((chips, *up), BF16), vm((chips, *down), BF16),
            vm((2, *up), BF16), vm(down, BF16), vm((2, 2, *up), BF16), vm((2, *down), BF16),
            vm((2, 2, rows // 2, ff_chunk), BF16), vm((2, LANES // 2, d), BF16), vm((2, 2, *up), BF16), vm((2, *down), BF16),
            vm((2, *up), BF16), vm(down, BF16),
            dma((units, 3, 14)), dma((units, 3, 14)), dma((3, units, n)), dma((3, units)), dma((2, 3)), dma((2,)),
            dma((3,)), dma((3,)), dma((3, 2)), dma((3, 2)), dma((3, 2)), dma((3, 2)), dma((3, n)),
            pltpu.SemaphoreType.REGULAR((3,)),
        ]
        outs = pl.pallas_call(
            functools.partial(kernel, size),
            out_shape=[
                sds(x.shape, BF16), sds(wg.shape, BF16), sds(wu.shape, BF16), sds(wd.shape, BF16),
                sds((units, d, ff_chunk), BF16), sds((units, d, ff_chunk), BF16), sds((units, ff_chunk, d), BF16),
            ],
            in_specs=[hbm] * 5,
            out_specs=[hbm] * 7,
            scratch_shapes=scratch,
            compiler_params=pltpu.CompilerParams(
                collective_id=0, has_side_effects=True, vmem_limit_bytes=67_043_328),
            name="stack",
        )(x, dy, wg, wu, wd)
        return tuple(outs[:4])

    seq, w = P(("rep", "dp"), None, None), P(None, "dp", None)
    return jax.shard_map(step, mesh=mesh, in_specs=(seq, seq, w, w, w),
                         out_specs=(seq, *(P("rep", "dp", None),) * 3), check_vma=False)
```

```python
import functools

import jax
import jax.numpy as jnp
from jax import lax
from jax.experimental import pallas as pl
from jax.experimental.pallas import tpu as pltpu
from jax.sharding import PartitionSpec as P

MESH = pl.DeviceIdType.MESH
F32, BF16 = jnp.float32, jnp.bfloat16
LANES = 128
NT = (((1,), (1,)), ((), ()))
G, U, D = range(3)
PIECES = (8, 1, 1, 1)


def dot(a, b, dims=(((1,), (0,)), ((), ()))):
    return lax.dot_general(a, b, dims, preferred_element_type=F32)


def loop(n, body, unroll=1):
    def step(i, carry):
        body(i)
        return carry

    lax.fori_loop(0, n, step, 0, unroll=unroll)


def kernel(size, x_hbm, dy_hbm, wg_hbm, wu_hbm, wd_hbm,
           dx_hbm, og_hbm, ou_hbm, od_hbm, fg, fu, fd, kept,
           own_g, own_u, own_d, sgu, sd, h, a, at, dout, dt, da, act, dgu,
           pg, pu, pd, sib_g, sib_u, sib_d, send_a_g, send_a_d, send_b_g, send_b_d,
           ra_g, ra_d, rb_g, rb_d, out_g, out_d,
           ag_send, ag_recv, own_sem, own_out, slot_sem, in_sem,
           sib_send, sib_recv, a_send, a_recv, b_send, b_recv, out_sem, keep_sem, credit):
    layers, chunks, rows, d, ff_chunk, tokens = (
        size[k] for k in ("layers", "chunks", "rows", "d", "ff_chunk", "tokens"))
    n = size["n"]
    chips = n // 2
    me = lax.axis_index("dp")
    x, c = me // 2, me % 2
    xr, xl, xo = lax.rem(x + 1, chips), lax.rem(x + chips - 1, chips), lax.rem(x + 2, chips)
    right, left, sibling = {"dp": xr * 2 + c}, {"dp": xl * 2 + c}, {"dp": x * 2 + 1 - c}
    units = layers * chunks

    barrier = pltpu.get_barrier_semaphore()
    other = {"rep": lax.axis_index("rep") + 1 - 2 * (lax.axis_index("rep") % 2)}
    for who in (left, right, sibling, other):
        pl.semaphore_signal(barrier, inc=1, device_id=who, device_id_type=MESH)

    R = (rows, rows, LANES)
    own, full = (own_g, own_u, own_d), (fg, fu, fd)
    sg, su = (sgu.at[:, :, pl.ds(i * ff_chunk, ff_chunk)] for i in range(2))
    dg, du = (dgu.at[:, pl.ds(i * ff_chunk, ff_chunk)] for i in range(2))
    slot = (sg, su, sd)

    def own_copies(q, m):
        l, k = q // chunks, q % chunks
        if m == D:
            return [pltpu.make_async_copy(wd_hbm.at[l, pl.ds(k * LANES, LANES)], own_d.at[q], own_sem.at[m, q, 0])]
        src = (wg_hbm, wu_hbm)[m]
        return [pltpu.make_async_copy(
            src.at[l, :, pl.ds((j * chunks + k) * LANES, LANES)], own[m].at[q, :, pl.ds(j * LANES, LANES)],
            own_sem.at[m, q, j]) for j in range(n)]

    def load_x(dst):
        return pltpu.make_async_copy(x_hbm.at[0], dst, in_sem.at[0])

    load_dy = pltpu.make_async_copy(dy_hbm.at[0], dout, in_sem.at[1])

    S = tuple(r // 3 // 16 * 16 for r in R)
    pair = lax.axis_index("rep") % 2
    partner = {"rep": lax.axis_index("rep") + 1 - 2 * pair}

    def block(q, m, owner, start, count):
        return full[m].at[q, pl.ds(pl.multiple_of(owner * R[m] + start, 16), count)]

    def gather_copy(q, m, i):
        to = (right, left, sibling, right, sibling, left, sibling, sibling,
              partner, partner, partner, sibling, sibling, sibling)[i]
        ours, both = pair * S[m], R[m] - S[m]
        if i < 2:
            src, dst = own[m].at[q, pl.ds(pl.multiple_of(ours, 16), both)], block(q, m, me, ours, both)
        elif i == 2:
            src, dst = own[m].at[q], block(q, m, me, 0, R[m])
        else:
            owner = (xl, xl, xr, xr, xo, xl, xr, xo, xl, xr, xo)[i - 3] * 2 + c
            if i == 3:
                piece = (ours, both // 2)
            elif i == 5:
                piece = (ours + both // 2, both // 2)
            elif i < 8:
                piece = (ours, both)
            elif i < 11:
                piece = (pair * both, S[m])
            else:
                piece = ((1 - pair) * both, S[m])
            src = dst = block(q, m, owner, *piece)
        return pltpu.make_async_remote_copy(src, dst, ag_send.at[q, m, i], ag_recv.at[q, m, i],
                                            device_id=to, device_id_type=MESH)

    def own_store(q, m):
        return pltpu.make_async_copy(own[m].at[q], block(q, m, me, 0, R[m]), own_out.at[m, q])

    def g0(q):
        for m in range(3):
            for i in range(3):
                gather_copy(q, m, i).start()
            own_store(q, m).start()

    def g1(q, m):
        for came in range(2):
            gather_copy(q, m, came).wait_recv()
            for i in (3 + 2 * came, 8 + came, 4 + 2 * came):
                gather_copy(q, m, i).start()

    def g2(q, m):
        gather_copy(q, m, 3).wait_recv()
        gather_copy(q, m, 5).wait_recv()
        gather_copy(q, m, 10).start()
        gather_copy(q, m, 7).start()

    def g3(q, m):
        for i in range(3):
            gather_copy_from_partner(q, m, i).wait_recv()
            gather_copy(q, m, 11 + i).start()

    def gather_copy_from_partner(q, m, i):
        owner = (xl, xr, xo)[i] * 2 + c
        piece = block(q, m, owner, (1 - pair) * (R[m] - S[m]), S[m])
        return pltpu.make_async_remote_copy(piece, piece, ag_send.at[q, m, 8 + i], ag_recv.at[q, m, 8 + i],
                                            device_id=partner, device_id_type=MESH)

    def g4(q):
        for m in range(3):
            for i in (2, 4, 6, 7, 11, 12, 13):
                gather_copy(q, m, i).wait_recv()
            own_store(q, m).wait()

    def g_end(q, m):
        for i in range(14):
            gather_copy(q, m, i).wait_send()

    last = units - 1

    def gather_part(q, i):
        if i == 1:
            @pl.when(q < last)
            def _():
                g1(q, D)
                g0(q + 1)
        elif 2 <= i < 5:
            g2(q, i - 2)
        elif i >= 5:
            g3(q, i - 5)

            if i == 6:
                @pl.when(q < last)
                def _():
                    g1(q + 1, G)

    def gather_end(q, s):
        g4(q)
        for m in range(3):
            fetch(q, s, m).start()

        @pl.when(q < last - 1)
        def _():
            g1(q + 1, U)

    def fetch(q, s, m):
        return pltpu.make_async_copy(full[m].at[q], slot[m].at[s], slot_sem.at[s, m])

    TP = 256
    prep_tiles = tokens // TP

    def scale_of(wide):
        return lax.rsqrt(jnp.mean(wide * wide, -1, keepdims=True) + 1e-6)

    def norm_tile(i, src=h):
        r = pl.ds(i * TP, TP)
        wide = src[r, :].astype(F32)
        a_tile = (wide * scale_of(wide)).astype(BF16)
        a[r, :] = a_tile
        return a_tile

    def transpose_a(i):
        cols = pl.ds(pl.multiple_of(i * TP, TP), TP)
        at[:, cols] = norm_tile(i).T

    def restart(i):
        r = pl.ds(i * TP, TP)
        cols = pl.ds(pl.multiple_of(i * TP, TP), TP)
        h[r, :] = a[r, :]
        at[:, cols] = norm_tile(i, a).T
        dt[:, cols] = dout[r, :].T

    def transpose_dout(i):
        cols = pl.ds(pl.multiple_of(i * TP, TP), TP)
        dt[:, cols] = dout[pl.ds(i * TP, TP), :].T

    T, NB = 512, 1024
    TI = 512
    TH, NH = 1024, 256
    strips = ff_chunk // NH
    spots = strips * (tokens // TH)
    tiles, blocks = tokens // T, ff_chunk // NB

    def forward_tile(s, i, first):
        r = pl.ds(i * T, T)
        a_tile = a[r, :]
        gate = dot(a_tile, sg[s])
        up = dot(a_tile, su[s])
        hidden = (gate * jax.nn.sigmoid(gate) * up).astype(BF16)
        term = dot(hidden, sd[s])

        da[r, :] = jnp.where(first, 0.0, da[r, :]) + term

    def hidden_tile(s, i, b):
        r = pl.ds(pl.multiple_of(i * TH, TH), TH)
        f = pl.ds(pl.multiple_of(b * NH, NH), NH)
        a_tile = a[r, :]
        gate = dot(a_tile, sg[s, :, f])
        up = dot(a_tile, su[s, :, f])
        by_hidden = dot(dout[r, :], sd[s, f, :], NT).astype(BF16).astype(F32)
        sig = jax.nn.sigmoid(gate)
        silu = gate * sig
        act[r, f] = (silu * up).astype(BF16)
        du[r, f] = (by_hidden * silu).astype(BF16)
        dg[r, f] = (by_hidden * up * (sig + silu * (1.0 - sig))).astype(BF16)

    def weights_up(b, src, dst):
        f = pl.ds(pl.multiple_of(b * NB, NB), NB)
        term = dot(at[...], src[:, f]).astype(BF16)
        dst[:, :, f] = term.reshape(chips, 2 * rows, NB)

    def weights_down(b):
        f = pl.ds(pl.multiple_of(b * NB, NB), NB)
        term = dot(dt[...], act[:, f])
        per = NB // (2 * LANES)
        pd[pl.ds(b * per, per)] = term.T.astype(BF16).reshape(per, 2 * LANES, d)

    def input_tile(s, i, first):
        r = pl.ds(i * TI, TI)
        term = dot(dgu[r, :], sgu[s], NT)

        da[r, :] = jnp.where(first, 0.0, da[r, :]) + term

    def norm_back(i):
        r = pl.ds(i * TP, TP)
        wide = h[r, :].astype(F32)
        s = scale_of(wide)
        g = da[r, :].astype(BF16).astype(F32)
        along = jnp.sum(g * wide, -1, keepdims=True)
        back = (g * s - wide * (s * s * s * along * (1.0 / d))).astype(BF16)
        dout[r, :] = (dout[r, :].astype(F32) + back.astype(F32)).astype(BF16)

    keep = pltpu.make_async_copy(dgu, kept, keep_sem.at[tokens // TI])

    def again(i):
        r = pl.ds(i * TI, TI)
        return pltpu.make_async_copy(kept.at[r], dgu.at[r], keep_sem.at[i])

    part, sib = (pg, pu, pd), (sib_g, sib_u, sib_d)
    view = lambda pair, m: pair[0].at[m] if m != D else pair[1]
    sa = [view((send_a_g, send_a_d), m) for m in range(3)]
    ra = [[r_.at[i] for i in range(2)] for r_ in (view((ra_g, ra_d), m) for m in range(3))]
    sb = [[r_.at[i] for i in range(2)] for r_ in (view((send_b_g, send_b_d), m) for m in range(3))]
    rb = [[r_.at[i] for i in range(2)] for r_ in (view((rb_g, rb_d), m) for m in range(3))]
    out = [view((out_g, out_d), m) for m in range(3)]

    def rs_sib(m):
        return pltpu.make_async_remote_copy(
            part[m].at[:, pl.ds(pl.multiple_of((1 - c) * R[m], 16), R[m])], sib[m], sib_send.at[m], sib_recv.at[m],
            device_id=sibling, device_id_type=MESH)

    def rs_a(m, i):
        half = R[m] // 2
        return pltpu.make_async_remote_copy(
            sa[m].at[pl.ds(i * half, half)], ra[m][i], a_send.at[m, i], a_recv.at[m, i],
            device_id=(right, left)[i], device_id_type=MESH)

    def rs_b(m, i):
        return pltpu.make_async_remote_copy(
            sb[m][i], rb[m][i], b_send.at[m, i], b_recv.at[m, i],
            device_id=(right, left)[i], device_id_type=MESH)

    def term(m, chip):
        mine = part[m][chip, pl.ds(pl.multiple_of(c * R[m], 16), R[m]), :]
        return mine.astype(F32) + sib[m][chip].astype(F32)

    def rs1(s, m):
        @pl.when(s > 0)
        def _():
            pl.semaphore_wait(credit.at[m], 1)

        rs_sib(m).start()

    def rs2(s, m):
        rs_sib(m).wait()
        sa[m][...] = term(m, xo).astype(BF16)
        for i in range(2):
            rs_a(m, i).start()

    def rs3(m):
        half = R[m] // 2
        for i in range(2):
            rs_a(m, i).wait()
        for i, chip in enumerate((xr, xl)):
            whole = term(m, chip)
            came = ra[m][i][...].astype(F32)
            top, low = whole[:half], whole[half:]
            if i == 0:
                top = top + came
            else:
                low = low + came
            sb[m][i][:half, :] = top.astype(BF16)
            sb[m][i][half:, :] = low.astype(BF16)
        for i in range(2):
            rs_b(m, i).start()

    def reduce_part(s, j):
        if j == 0:
            rs2(s, D)
        rs3(j)

    def out_copies(s, m):
        l, k = layers - 1 - s // chunks, lax.rem(s, chunks)
        if m == D:
            return [pltpu.make_async_copy(out[m], od_hbm.at[l, pl.ds(k * LANES, LANES)], out_sem.at[m, 0])]
        dst = (og_hbm, ou_hbm)[m]
        return [pltpu.make_async_copy(
            out[m].at[:, pl.ds(j * LANES, LANES)],
            dst.at[l, :, pl.ds(pl.multiple_of((j * chunks + k) * LANES, LANES), LANES)], out_sem.at[m, j])
            for j in range(n)]

    def rs4(s, m):
        @pl.when(s > 0)
        def _():
            for cp in out_copies(s, m):
                cp.wait()

        for i in range(2):
            rs_b(m, i).wait()
        total = term(m, x) + rb[m][0][...].astype(F32) + rb[m][1][...].astype(F32)
        out[m][...] = total.astype(BF16)
        for cp in out_copies(s, m):
            cp.start()

        @pl.when(s < units - 1)
        def _():
            pl.semaphore_signal(credit.at[m], inc=1, device_id=sibling, device_id_type=MESH)

    for m in range(3):
        for cp in own_copies(0, m):
            cp.start()
    load_x(h).start()
    load_dy.start()
    for m in range(3):
        for cp in own_copies(0, m):
            cp.wait()
    pl.semaphore_wait(barrier, 4)
    g0(0)
    for q in range(1, units):
        for m in range(3):
            for cp in own_copies(q, m):
                cp.start()
    for q in range(1, units):
        for m in range(3):
            for cp in own_copies(q, m):
                cp.wait()
    load_x(h).wait()
    loop(prep_tiles, norm_tile)
    load_dy.wait()
    loop(prep_tiles, transpose_dout)
    g1(0, G)
    g1(0, U)
    for i in range(8):
        gather_part(0, i)
    gather_end(0, 0)

    def forward(k, carry):
        s = lax.rem(k, 2)
        for m in range(3):
            fetch(k, s, m).wait()

        def tile(i):
            for j in range(8):
                @pl.when(i == j * tiles // 8)
                def _():
                    gather_part(k + 1, j)

            forward_tile(s, i, k == 0)

        loop(tiles, tile)
        gather_end(k + 1, 1 - s)
        return carry

    fwd = units - chunks
    lax.fori_loop(0, fwd, forward, 0)

    def add_hidden(i):
        r = pl.ds(i * TP, TP)
        h[r, :] = (h[r, :].astype(F32) + da[r, :].astype(BF16).astype(F32)).astype(BF16)

    loop(prep_tiles, add_hidden)
    loop(prep_tiles, transpose_a)

    def backward(k, carry):
        s = lax.rem(k + fwd, 2)
        q_next = lax.rem(k + fwd + 1, units)
        more = k < units - fwd - 1
        first = lax.rem(k, chunks) == 0

        @pl.when(jnp.logical_and(first, k > 0))
        def _():
            load_x(a).wait()
            loop(prep_tiles, restart)

        for m in range(3):
            fetch(0, s, m).wait()

        @pl.when(k == units - 1)
        def _():
            keep.wait()

        def strip(b):
            for j in range(8):
                @pl.when(jnp.logical_and(more, b == j * strips // 8))
                def _():
                    gather_part(q_next, j)

            for j in range(3):
                @pl.when(jnp.logical_and(k == units - 1, b == j))
                def _():
                    reduce_part(k - 1, j)

            for i in range(tokens // TH):
                hidden_tile(s, i, b)

        loop(strips, strip)

        @pl.when(k == units - 2)
        def _():
            keep.start()

        def done(m):
            @pl.when(k > 0)
            def _():
                rs4(k - 1, m)

        @pl.when(jnp.logical_and(lax.rem(k, chunks) == chunks - 1, k < units - 1))
        def _():
            load_x(a).start()

        done(G)
        loop(blocks, lambda b: weights_up(b, dg, pg))
        rs1(k, G)

        @pl.when(jnp.logical_and(more, q_next == last - 1))
        def _():
            g1(last, U)
            g1(last, D)

        done(U)
        loop(blocks, lambda b: weights_up(b, du, pu))
        rs1(k, U)
        rs2(k, G)

        done(D)
        loop(blocks, weights_down)
        rs1(k, D)
        rs2(k, U)

        @pl.when(more)
        def _():
            gather_end(q_next, 1 - s)

        @pl.when(jnp.logical_and(k < units - 1, jnp.logical_not(more)))
        def _():
            for m in range(3):
                fetch(q_next, 1 - s, m).start()

        @pl.when(k != units - 2)
        def _():
            def back(i):
                for j in range(2):
                    @pl.when(i == j + 1)
                    def _():
                        reduce_part(k, j)

                input_tile(s, i, first)

                @pl.when(k == units - 1)
                def _():
                    again(i).start()

            loop(tokens // TI, back)
            reduce_part(k, 2)

        @pl.when(k == units - 1)
        def _():
            def rest(i):
                again(i).wait()
                input_tile(1 - s, i, False)

            loop(tokens // TI, rest)

        @pl.when(lax.rem(k, chunks) == chunks - 1)
        def _():
            loop(prep_tiles, norm_back)


        return carry

    lax.fori_loop(0, units, backward, 0)
    store_dx = pltpu.make_async_copy(dout, dx_hbm.at[0], in_sem.at[1])
    store_dx.start()
    for m in range(3):
        rs4(units - 1, m)
    for m in range(3):
        for cp in out_copies(units - 1, m):
            cp.wait()
    store_dx.wait()

    def ends(q):
        for m in range(3):
            g_end(q, m)

    loop(units, ends)


def finish(arrays):
    def copy_all(*refs):
        k = len(arrays)
        ins, outs, held, (sem_in, sem_out) = refs[:k], refs[k:2 * k], refs[2 * k:3 * k], refs[3 * k:]
        pieces = []
        for j in range(k):
            rows = arrays[j].shape[1] // PIECES[j]
            pieces += [(j, l, pl.ds(p * rows, rows)) for l in range(arrays[j].shape[0]) for p in range(PIECES[j])]
        into = [pltpu.make_async_copy(ins[j].at[l, r], held[j].at[l, r], sem_in.at[i]) for i, (j, l, r) in enumerate(pieces)]
        back = [pltpu.make_async_copy(held[j].at[l, r], outs[j].at[l, r], sem_out.at[i]) for i, (j, l, r) in enumerate(pieces)]
        for cp in into:
            cp.start()
        for a, b in zip(into, back):
            a.wait()
            b.start()
        for b in back:
            b.wait()

    hbm = pl.BlockSpec(memory_space=pl.ANY)
    count = sum(a.shape[0] * p for a, p in zip(arrays, PIECES))
    return tuple(pl.pallas_call(
        copy_all,
        out_shape=[jax.ShapeDtypeStruct(a.shape, a.dtype) for a in arrays],
        in_specs=[hbm] * len(arrays),
        out_specs=[hbm] * len(arrays),
        scratch_shapes=[pltpu.VMEM(a.shape, a.dtype) for a in arrays] + [pltpu.SemaphoreType.DMA((count,))] * 2,
        compiler_params=pltpu.CompilerParams(vmem_limit_bytes=67_043_328),
        name="finish",
    )(*arrays))


def solution(mesh):
    n = mesh.shape["dp"]

    def step(x, dy, wg, wu, wd):
        layers, rows, ff = wg.shape
        tokens, d = x.shape[1:]
        chunks = ff // (n * LANES)
        ff_chunk = n * LANES
        units = layers * chunks
        chips = n // 2
        size = dict(layers=layers, chunks=chunks, rows=rows, d=d, ff_chunk=ff_chunk, tokens=tokens, n=n)
        sds = jax.ShapeDtypeStruct
        vm = pltpu.VMEM
        dma = pltpu.SemaphoreType.DMA
        hbm = pl.BlockSpec(memory_space=pl.ANY)
        td = (tokens, d)
        tf = (tokens, ff_chunk)
        up, down = (rows, ff_chunk), (LANES, d)
        scratch = [
            vm((units, *up), BF16), vm((units, *up), BF16), vm((units, *down), BF16),
            vm((2, d, 2 * ff_chunk), BF16), vm((2, ff_chunk, d), BF16),
            vm(td, BF16), vm(td, BF16), vm(td[::-1], BF16), vm(td, BF16), vm(td[::-1], BF16), vm(td, F32),
            vm(tf, BF16), vm((tokens, 2 * ff_chunk), BF16),
            vm((chips, 2 * rows, ff_chunk), BF16), vm((chips, 2 * rows, ff_chunk), BF16), vm((chips, 2 * LANES, d), BF16),
            vm((chips, *up), BF16), vm((chips, *up), BF16), vm((chips, *down), BF16),
            vm((2, *up), BF16), vm(down, BF16), vm((2, 2, *up), BF16), vm((2, *down), BF16),
            vm((2, 2, rows // 2, ff_chunk), BF16), vm((2, LANES // 2, d), BF16), vm((2, 2, *up), BF16), vm((2, *down), BF16),
            vm((2, *up), BF16), vm(down, BF16),
            dma((units, 3, 14)), dma((units, 3, 14)), dma((3, units, n)), dma((3, units)), dma((2, 3)), dma((2,)),
            dma((3,)), dma((3,)), dma((3, 2)), dma((3, 2)), dma((3, 2)), dma((3, 2)), dma((3, n)), dma((tokens // 512 + 1,)),
            pltpu.SemaphoreType.REGULAR((3,)),
        ]
        outs = pl.pallas_call(
            functools.partial(kernel, size),
            out_shape=[
                sds(x.shape, BF16), sds(wg.shape, BF16), sds(wu.shape, BF16), sds(wd.shape, BF16),
                sds((units, d, ff_chunk), BF16), sds((units, d, ff_chunk), BF16), sds((units, ff_chunk, d), BF16),
                sds((tokens, 2 * ff_chunk), BF16),
            ],
            in_specs=[hbm] * 5,
            out_specs=[hbm] * 8,
            scratch_shapes=scratch,
            compiler_params=pltpu.CompilerParams(
                collective_id=0, has_side_effects=True, vmem_limit_bytes=67_043_328),
            name="stack",
        )(x, dy, wg, wu, wd)
        return finish(outs[:4])

    seq, w = P(("rep", "dp"), None, None), P(None, "dp", None)
    return jax.shard_map(step, mesh=mesh, in_specs=(seq, seq, w, w, w),
                         out_specs=(seq, *(P("rep", "dp", None),) * 3), check_vma=False)
```

```python
import functools

import jax
import jax.numpy as jnp
from jax import lax
from jax.experimental import pallas as pl
from jax.experimental.pallas import tpu as pltpu
from jax.sharding import PartitionSpec as P

MESH = pl.DeviceIdType.MESH
F32, BF16 = jnp.float32, jnp.bfloat16
LANES = 128
NT = (((1,), (1,)), ((), ()))
G, U, D = range(3)
PIECES = (8, 1, 1, 1)


def dot(a, b, dims=(((1,), (0,)), ((), ()))):
    return lax.dot_general(a, b, dims, preferred_element_type=F32)


def loop(n, body, unroll=1):
    def step(i, carry):
        body(i)
        return carry

    lax.fori_loop(0, n, step, 0, unroll=unroll)


def kernel(size, x_hbm, dy_hbm, wg_hbm, wu_hbm, wd_hbm,
           dx_hbm, og_hbm, ou_hbm, od_hbm, fg, fu, fd, kept,
           own_g, own_u, own_d, sgu, sd, h, a, at, dout, dt, da, act, dgu,
           pg, pu, pd, sib_g, sib_u, sib_d, send_a_g, send_a_d, send_b_g, send_b_d,
           ra_g, ra_d, rb_g, rb_d, out_g, out_d,
           ag_send, ag_recv, own_sem, own_out, slot_sem, in_sem,
           sib_send, sib_recv, a_send, a_recv, b_send, b_recv, out_sem, keep_sem, credit):
    layers, chunks, rows, d, ff_chunk, tokens = (
        size[k] for k in ("layers", "chunks", "rows", "d", "ff_chunk", "tokens"))
    n = size["n"]
    chips = n // 2
    me = lax.axis_index("dp")
    x, c = me // 2, me % 2
    xr, xl, xo = lax.rem(x + 1, chips), lax.rem(x + chips - 1, chips), lax.rem(x + 2, chips)
    right, left, sibling = {"dp": xr * 2 + c}, {"dp": xl * 2 + c}, {"dp": x * 2 + 1 - c}
    units = layers * chunks

    barrier = pltpu.get_barrier_semaphore()
    other = {"rep": lax.axis_index("rep") + 1 - 2 * (lax.axis_index("rep") % 2)}
    for who in (left, right, sibling, other):
        pl.semaphore_signal(barrier, inc=1, device_id=who, device_id_type=MESH)

    R = (rows, rows, LANES)
    own, full = (own_g, own_u, own_d), (fg, fu, fd)
    sg, su = (sgu.at[:, :, pl.ds(i * ff_chunk, ff_chunk)] for i in range(2))
    dg, du = (dgu.at[:, pl.ds(i * ff_chunk, ff_chunk)] for i in range(2))
    slot = (sg, su, sd)

    def own_copies(q, m):
        l, k = q // chunks, q % chunks
        if m == D:
            return [pltpu.make_async_copy(wd_hbm.at[l, pl.ds(k * LANES, LANES)], own_d.at[q], own_sem.at[m, q, 0])]
        src = (wg_hbm, wu_hbm)[m]
        return [pltpu.make_async_copy(
            src.at[l, :, pl.ds((j * chunks + k) * LANES, LANES)], own[m].at[q, :, pl.ds(j * LANES, LANES)],
            own_sem.at[m, q, j]) for j in range(n)]

    def load_x(dst):
        return pltpu.make_async_copy(x_hbm.at[0], dst, in_sem.at[0])

    load_dy = pltpu.make_async_copy(dy_hbm.at[0], dout, in_sem.at[1])

    S = tuple(r // 3 // 16 * 16 for r in R)
    pair = lax.axis_index("rep") % 2
    partner = {"rep": lax.axis_index("rep") + 1 - 2 * pair}

    def block(q, m, owner, start, count):
        return full[m].at[q, pl.ds(pl.multiple_of(owner * R[m] + start, 16), count)]

    def gather_copy(q, m, i):
        to = (right, left, sibling, right, sibling, left, sibling, sibling,
              partner, partner, partner, sibling, sibling, sibling)[i]
        ours, both = pair * S[m], R[m] - S[m]
        if i < 2:
            src, dst = own[m].at[q, pl.ds(pl.multiple_of(ours, 16), both)], block(q, m, me, ours, both)
        elif i == 2:
            src, dst = own[m].at[q], block(q, m, me, 0, R[m])
        else:
            owner = (xl, xl, xr, xr, xo, xl, xr, xo, xl, xr, xo)[i - 3] * 2 + c
            if i == 3:
                piece = (ours, both // 2)
            elif i == 5:
                piece = (ours + both // 2, both // 2)
            elif i < 8:
                piece = (ours, both)
            elif i < 11:
                piece = (pair * both, S[m])
            else:
                piece = ((1 - pair) * both, S[m])
            src = dst = block(q, m, owner, *piece)
        return pltpu.make_async_remote_copy(src, dst, ag_send.at[q, m, i], ag_recv.at[q, m, i],
                                            device_id=to, device_id_type=MESH)

    def own_store(q, m):
        return pltpu.make_async_copy(own[m].at[q], block(q, m, me, 0, R[m]), own_out.at[m, q])

    def g0(q):
        for m in range(3):
            for i in range(3):
                gather_copy(q, m, i).start()
            own_store(q, m).start()

    def g1(q, m):
        for came in range(2):
            gather_copy(q, m, came).wait_recv()
            for i in (3 + 2 * came, 8 + came, 4 + 2 * came):
                gather_copy(q, m, i).start()

    def g2(q, m):
        gather_copy(q, m, 3).wait_recv()
        gather_copy(q, m, 5).wait_recv()
        gather_copy(q, m, 10).start()
        gather_copy(q, m, 7).start()

    def g3(q, m):
        for i in range(3):
            gather_copy_from_partner(q, m, i).wait_recv()
            gather_copy(q, m, 11 + i).start()

    def gather_copy_from_partner(q, m, i):
        owner = (xl, xr, xo)[i] * 2 + c
        piece = block(q, m, owner, (1 - pair) * (R[m] - S[m]), S[m])
        return pltpu.make_async_remote_copy(piece, piece, ag_send.at[q, m, 8 + i], ag_recv.at[q, m, 8 + i],
                                            device_id=partner, device_id_type=MESH)

    def g4(q):
        for m in range(3):
            for i in (2, 4, 6, 7, 11, 12, 13):
                gather_copy(q, m, i).wait_recv()
            own_store(q, m).wait()

    def g_end(q, m):
        for i in range(14):
            gather_copy(q, m, i).wait_send()

    last = units - 1

    def gather_part(q, i):
        if i == 1:
            @pl.when(q < last)
            def _():
                g1(q, D)
                g0(q + 1)
        elif 2 <= i < 5:
            g2(q, i - 2)
        elif i >= 5:
            g3(q, i - 5)

            if i == 6:
                @pl.when(q < last)
                def _():
                    g1(q + 1, G)

    def gather_end(q, s):
        g4(q)
        for m in range(3):
            fetch(q, s, m).start()

        @pl.when(q < last - 1)
        def _():
            g1(q + 1, U)

    def fetch(q, s, m):
        return pltpu.make_async_copy(full[m].at[q], slot[m].at[s], slot_sem.at[s, m])

    TP = 256
    prep_tiles = tokens // TP

    def scale_of(wide):
        return lax.rsqrt(jnp.mean(wide * wide, -1, keepdims=True) + 1e-6)

    def normed(wide, r):
        a_tile = (wide * scale_of(wide)).astype(BF16)
        a[r, :] = a_tile
        return a_tile

    def norm_tile(i):
        r = pl.ds(i * TP, TP)
        normed(h[r, :].astype(F32), r)

    def transpose_dout(i):
        cols = pl.ds(pl.multiple_of(i * TP, TP), TP)
        dt[:, cols] = dout[pl.ds(i * TP, TP), :].T

    T, NB = 512, 1024
    TI = 512
    TH, NH = 1024, 256
    strips = ff_chunk // NH
    spots = strips * (tokens // TH)
    tiles, blocks = tokens // T, ff_chunk // NB

    def forward_tile(s, i, first):
        r = pl.ds(i * T, T)
        a_tile = a[r, :]
        gate = dot(a_tile, sg[s])
        up = dot(a_tile, su[s])
        hidden = (gate * jax.nn.sigmoid(gate) * up).astype(BF16)
        term = dot(hidden, sd[s])

        da[r, :] = jnp.where(first, 0.0, da[r, :]) + term

    def hidden_tile(s, i, b):
        r = pl.ds(pl.multiple_of(i * TH, TH), TH)
        f = pl.ds(pl.multiple_of(b * NH, NH), NH)
        a_tile = a[r, :]
        gate = dot(a_tile, sg[s, :, f])
        up = dot(a_tile, su[s, :, f])
        by_hidden = dot(dout[r, :], sd[s, f, :], NT).astype(BF16).astype(F32)
        sig = jax.nn.sigmoid(gate)
        silu = gate * sig
        act[r, f] = (silu * up).astype(BF16)
        du[r, f] = (by_hidden * silu).astype(BF16)
        dg[r, f] = (by_hidden * up * (sig + silu * (1.0 - sig))).astype(BF16)

    def weights_up(b, src, dst):
        f = pl.ds(pl.multiple_of(b * NB, NB), NB)
        term = dot(at[...], src[:, f]).astype(BF16)
        dst[:, :, f] = term.reshape(chips, 2 * rows, NB)

    def weights_down(b):
        f = pl.ds(pl.multiple_of(b * NB, NB), NB)
        term = dot(dt[...], act[:, f])
        per = NB // (2 * LANES)
        pd[pl.ds(b * per, per)] = term.T.astype(BF16).reshape(per, 2 * LANES, d)

    def input_tile(s, i, first):
        r = pl.ds(i * TI, TI)
        term = dot(dgu[r, :], sgu[s], NT)

        da[r, :] = jnp.where(first, 0.0, da[r, :]) + term

    def norm_back(i):
        r = pl.ds(i * TP, TP)
        wide = h[r, :].astype(F32)
        s = scale_of(wide)
        g = da[r, :].astype(BF16).astype(F32)
        along = jnp.sum(g * wide, -1, keepdims=True)
        back = (g * s - wide * (s * s * s * along * (1.0 / d))).astype(BF16)
        by_input = (dout[r, :].astype(F32) + back.astype(F32)).astype(BF16)
        dout[r, :] = by_input
        return by_input

    def next_layer(i):
        r = pl.ds(i * TP, TP)
        cols = pl.ds(pl.multiple_of(i * TP, TP), TP)
        dt[:, cols] = norm_back(i).T
        came = a[r, :]
        h[r, :] = came
        at[:, cols] = normed(came.astype(F32), r).T

    keep = pltpu.make_async_copy(dgu, kept, keep_sem.at[tokens // TI])

    def again(i):
        r = pl.ds(i * TI, TI)
        return pltpu.make_async_copy(kept.at[r], dgu.at[r], keep_sem.at[i])

    part, sib = (pg, pu, pd), (sib_g, sib_u, sib_d)
    view = lambda pair, m: pair[0].at[m] if m != D else pair[1]
    sa = [view((send_a_g, send_a_d), m) for m in range(3)]
    ra = [[r_.at[i] for i in range(2)] for r_ in (view((ra_g, ra_d), m) for m in range(3))]
    sb = [[r_.at[i] for i in range(2)] for r_ in (view((send_b_g, send_b_d), m) for m in range(3))]
    rb = [[r_.at[i] for i in range(2)] for r_ in (view((rb_g, rb_d), m) for m in range(3))]
    out = [view((out_g, out_d), m) for m in range(3)]

    def rs_sib(m):
        return pltpu.make_async_remote_copy(
            part[m].at[:, pl.ds(pl.multiple_of((1 - c) * R[m], 16), R[m])], sib[m], sib_send.at[m], sib_recv.at[m],
            device_id=sibling, device_id_type=MESH)

    def rs_a(m, i):
        half = R[m] // 2
        return pltpu.make_async_remote_copy(
            sa[m].at[pl.ds(i * half, half)], ra[m][i], a_send.at[m, i], a_recv.at[m, i],
            device_id=(right, left)[i], device_id_type=MESH)

    def rs_b(m, i):
        return pltpu.make_async_remote_copy(
            sb[m][i], rb[m][i], b_send.at[m, i], b_recv.at[m, i],
            device_id=(right, left)[i], device_id_type=MESH)

    def term(m, chip):
        mine = part[m][chip, pl.ds(pl.multiple_of(c * R[m], 16), R[m]), :]
        return mine.astype(F32) + sib[m][chip].astype(F32)

    def rs1(s, m):
        @pl.when(s > 0)
        def _():
            pl.semaphore_wait(credit.at[m], 1)

        rs_sib(m).start()

    def rs2(s, m):
        rs_sib(m).wait()
        sa[m][...] = term(m, xo).astype(BF16)
        for i in range(2):
            rs_a(m, i).start()

    def rs3(m):
        half = R[m] // 2
        for i in range(2):
            rs_a(m, i).wait()
        for i, chip in enumerate((xr, xl)):
            whole = term(m, chip)
            came = ra[m][i][...].astype(F32)
            top, low = whole[:half], whole[half:]
            if i == 0:
                top = top + came
            else:
                low = low + came
            sb[m][i][:half, :] = top.astype(BF16)
            sb[m][i][half:, :] = low.astype(BF16)
        for i in range(2):
            rs_b(m, i).start()

    def reduce_part(s, j):
        if j == 0:
            rs2(s, D)
        rs3(j)

    def out_copies(s, m):
        l, k = layers - 1 - s // chunks, lax.rem(s, chunks)
        if m == D:
            return [pltpu.make_async_copy(out[m], od_hbm.at[l, pl.ds(k * LANES, LANES)], out_sem.at[m, 0])]
        dst = (og_hbm, ou_hbm)[m]
        return [pltpu.make_async_copy(
            out[m].at[:, pl.ds(j * LANES, LANES)],
            dst.at[l, :, pl.ds(pl.multiple_of((j * chunks + k) * LANES, LANES), LANES)], out_sem.at[m, j])
            for j in range(n)]

    def rs4(s, m):
        @pl.when(s > 0)
        def _():
            for cp in out_copies(s, m):
                cp.wait()

        for i in range(2):
            rs_b(m, i).wait()
        total = term(m, x) + rb[m][0][...].astype(F32) + rb[m][1][...].astype(F32)
        out[m][...] = total.astype(BF16)
        for cp in out_copies(s, m):
            cp.start()

        @pl.when(s < units - 1)
        def _():
            pl.semaphore_signal(credit.at[m], inc=1, device_id=sibling, device_id_type=MESH)

    for m in range(3):
        for cp in own_copies(0, m):
            cp.start()
    load_x(h).start()
    load_dy.start()
    for m in range(3):
        for cp in own_copies(0, m):
            cp.wait()
    pl.semaphore_wait(barrier, 4)
    g0(0)
    for q in range(1, units):
        for m in range(3):
            for cp in own_copies(q, m):
                cp.start()
    for q in range(1, units):
        for m in range(3):
            for cp in own_copies(q, m):
                cp.wait()
    load_x(h).wait()
    loop(prep_tiles, norm_tile)
    load_dy.wait()
    loop(prep_tiles, transpose_dout)
    g1(0, G)
    g1(0, U)
    for i in range(8):
        gather_part(0, i)
    gather_end(0, 0)

    def ends(q):
        for m in range(3):
            g_end(q, m)

    def forward(k, carry):
        s = lax.rem(k, 2)

        @pl.when(k > 0)
        def _():
            ends(k - 1)

        for m in range(3):
            fetch(k, s, m).wait()

        def tile(i):
            for j in range(8):
                @pl.when(i == j * tiles // 8)
                def _():
                    gather_part(k + 1, j)

            forward_tile(s, i, k == 0)

        loop(tiles, tile)
        gather_end(k + 1, 1 - s)
        return carry

    fwd = units - chunks
    lax.fori_loop(0, fwd, forward, 0)

    def add_hidden(i):
        r = pl.ds(i * TP, TP)
        cols = pl.ds(pl.multiple_of(i * TP, TP), TP)
        after = (h[r, :].astype(F32) + da[r, :].astype(BF16).astype(F32)).astype(BF16)
        h[r, :] = after
        at[:, cols] = normed(after.astype(F32), r).T

    loop(prep_tiles, add_hidden)

    def backward(k, carry):
        s = lax.rem(k + fwd, 2)
        q_next = lax.rem(k + fwd + 1, units)
        more = k < units - fwd - 1
        first = lax.rem(k, chunks) == 0

        for m in range(3):
            fetch(0, s, m).wait()

        @pl.when(jnp.logical_and(k < units - 1, jnp.logical_not(more)))
        def _():
            for m in range(3):
                fetch(q_next, 1 - s, m).start()

        @pl.when(k == units - 1)
        def _():
            keep.wait()

        def strip(b):
            for j, parts in enumerate(((0, 1), (2, 3, 4))):
                @pl.when(jnp.logical_and(more, b == j))
                def _():
                    for i in parts:
                        gather_part(q_next, i)

            for j, parts in enumerate(((0,), (1, 2))):
                @pl.when(jnp.logical_and(k == units - 1, b == j))
                def _():
                    for i in parts:
                        reduce_part(k - 1, i)

            for t in range(strips // 2):
                for i in range(tokens // TH):
                    hidden_tile(s, i, b * (strips // 2) + t)

        loop(2, strip)

        @pl.when(more)
        def _():
            for i in (5, 6, 7):
                gather_part(q_next, i)

        @pl.when(k == units - 2)
        def _():
            keep.start()

        def done(m):
            @pl.when(k > 0)
            def _():
                rs4(k - 1, m)

        @pl.when(jnp.logical_and(lax.rem(k, chunks) == chunks - 1, k < units - 1))
        def _():
            load_x(a).start()

        done(G)
        loop(blocks, lambda b: weights_up(b, dg, pg))
        rs1(k, G)

        @pl.when(jnp.logical_and(more, q_next == last - 1))
        def _():
            g1(last, U)
            g1(last, D)

        done(U)
        loop(blocks, lambda b: weights_up(b, du, pu))
        rs1(k, U)
        rs2(k, G)

        done(D)
        loop(blocks, weights_down)
        rs1(k, D)
        rs2(k, U)

        @pl.when(more)
        def _():
            gather_end(q_next, 1 - s)

        @pl.when(k != units - 2)
        def _():
            def back(i):
                for j in range(2):
                    @pl.when(i == 1 + 2 * j)
                    def _():
                        reduce_part(k, j)

                input_tile(s, i, first)

                @pl.when(k == units - 1)
                def _():
                    again(i).start()

            loop(tokens // TI, back)
            reduce_part(k, 2)

        @pl.when(k == units - 1)
        def _():
            def rest(i):
                again(i).wait()
                input_tile(1 - s, i, False)

            loop(tokens // TI, rest)

        @pl.when(lax.rem(k, chunks) == chunks - 1)
        def _():
            @pl.when(k < units - 1)
            def _():
                load_x(a).wait()
                loop(prep_tiles, next_layer)

            @pl.when(k == units - 1)
            def _():
                loop(prep_tiles, norm_back)


        return carry

    lax.fori_loop(0, units, backward, 0)
    store_dx = pltpu.make_async_copy(dout, dx_hbm.at[0], in_sem.at[1])
    store_dx.start()
    loop(units - fwd + 1, lambda q: ends(q + fwd - 1))
    for m in range(3):
        rs4(units - 1, m)
    for m in range(3):
        for cp in out_copies(units - 1, m):
            cp.wait()
    store_dx.wait()


def finish(arrays):
    def copy_all(*refs):
        k = len(arrays)
        ins, outs, held, (sem_in, sem_out) = refs[:k], refs[k:2 * k], refs[2 * k:3 * k], refs[3 * k:]
        pieces = []
        for j in range(k):
            rows = arrays[j].shape[1] // PIECES[j]
            pieces += [(j, l, pl.ds(p * rows, rows)) for l in range(arrays[j].shape[0]) for p in range(PIECES[j])]
        into = [pltpu.make_async_copy(ins[j].at[l, r], held[j].at[l, r], sem_in.at[i]) for i, (j, l, r) in enumerate(pieces)]
        back = [pltpu.make_async_copy(held[j].at[l, r], outs[j].at[l, r], sem_out.at[i]) for i, (j, l, r) in enumerate(pieces)]
        for cp in into:
            cp.start()
        for a, b in zip(into, back):
            a.wait()
            b.start()
        for b in back:
            b.wait()

    hbm = pl.BlockSpec(memory_space=pl.ANY)
    count = sum(a.shape[0] * p for a, p in zip(arrays, PIECES))
    return tuple(pl.pallas_call(
        copy_all,
        out_shape=[jax.ShapeDtypeStruct(a.shape, a.dtype) for a in arrays],
        in_specs=[hbm] * len(arrays),
        out_specs=[hbm] * len(arrays),
        scratch_shapes=[pltpu.VMEM(a.shape, a.dtype) for a in arrays] + [pltpu.SemaphoreType.DMA((count,))] * 2,
        compiler_params=pltpu.CompilerParams(vmem_limit_bytes=67_043_328),
        name="finish",
    )(*arrays))


def solution(mesh):
    n = mesh.shape["dp"]

    def step(x, dy, wg, wu, wd):
        layers, rows, ff = wg.shape
        tokens, d = x.shape[1:]
        chunks = ff // (n * LANES)
        ff_chunk = n * LANES
        units = layers * chunks
        chips = n // 2
        size = dict(layers=layers, chunks=chunks, rows=rows, d=d, ff_chunk=ff_chunk, tokens=tokens, n=n)
        sds = jax.ShapeDtypeStruct
        vm = pltpu.VMEM
        dma = pltpu.SemaphoreType.DMA
        hbm = pl.BlockSpec(memory_space=pl.ANY)
        td = (tokens, d)
        tf = (tokens, ff_chunk)
        up, down = (rows, ff_chunk), (LANES, d)
        scratch = [
            vm((units, *up), BF16), vm((units, *up), BF16), vm((units, *down), BF16),
            vm((2, d, 2 * ff_chunk), BF16), vm((2, ff_chunk, d), BF16),
            vm(td, BF16), vm(td, BF16), vm(td[::-1], BF16), vm(td, BF16), vm(td[::-1], BF16), vm(td, F32),
            vm(tf, BF16), vm((tokens, 2 * ff_chunk), BF16),
            vm((chips, 2 * rows, ff_chunk), BF16), vm((chips, 2 * rows, ff_chunk), BF16), vm((chips, 2 * LANES, d), BF16),
            vm((chips, *up), BF16), vm((chips, *up), BF16), vm((chips, *down), BF16),
            vm((2, *up), BF16), vm(down, BF16), vm((2, 2, *up), BF16), vm((2, *down), BF16),
            vm((2, 2, rows // 2, ff_chunk), BF16), vm((2, LANES // 2, d), BF16), vm((2, 2, *up), BF16), vm((2, *down), BF16),
            vm((2, *up), BF16), vm(down, BF16),
            dma((units, 3, 14)), dma((units, 3, 14)), dma((3, units, n)), dma((3, units)), dma((2, 3)), dma((2,)),
            dma((3,)), dma((3,)), dma((3, 2)), dma((3, 2)), dma((3, 2)), dma((3, 2)), dma((3, n)), dma((tokens // 512 + 1,)),
            pltpu.SemaphoreType.REGULAR((3,)),
        ]
        outs = pl.pallas_call(
            functools.partial(kernel, size),
            out_shape=[
                sds(x.shape, BF16), sds(wg.shape, BF16), sds(wu.shape, BF16), sds(wd.shape, BF16),
                sds((units, d, ff_chunk), BF16), sds((units, d, ff_chunk), BF16), sds((units, ff_chunk, d), BF16),
                sds((tokens, 2 * ff_chunk), BF16),
            ],
            in_specs=[hbm] * 5,
            out_specs=[hbm] * 8,
            scratch_shapes=scratch,
            compiler_params=pltpu.CompilerParams(
                collective_id=0, has_side_effects=True, vmem_limit_bytes=67_043_328),
            name="stack",
        )(x, dy, wg, wu, wd)
        return finish(outs[:4])

    seq, w = P(("rep", "dp"), None, None), P(None, "dp", None)
    return jax.shard_map(step, mesh=mesh, in_specs=(seq, seq, w, w, w),
                         out_specs=(seq, *(P("rep", "dp", None),) * 3), check_vma=False)
```
